256 devices in a mesh: expert: 128 (over x_hi, y, z, core), tensor: 2 (over x_lo).
Axes of the slice: x: 4 (x_hi: 2, x_lo: 2; x = x_hi * 2 + x_lo), y: 4, z: 8, core: 2. Of those that a mesh axis runs over, the one named last changes fastest.
Arguments:
- tokens: bfloat16 [65536, 768], P(('expert', 'tensor')), may hold values from -6 to 6
- norm_gain: float32 [768], replicated, may hold values from 0.25 to 1.75
- gates: float32 [65536], P(('expert', 'tensor')), may hold values from 0.25 to 1
- expert_ids: int32 [65536], P(('expert', 'tensor')), may hold values from 0 to 255, as said below
- slots: int32 [65536], P(('expert', 'tensor')), may hold values from -1 to 1, as said below
- w_in: bfloat16 [256, 768, 3072], P(('expert', 'tensor')), may hold values from -0.21875 to 0.21875
- w_out: bfloat16 [256, 768, 3072], P(('expert', 'tensor')), may hold values from -0.109375 to 0.109375
Outputs:
- mixed: bfloat16 [65536, 768], P(('expert', 'tensor'))
The draws below stay inside these ranges and needn't reach their ends.
Inputs may be any that keep to these rules, and one draw needn't show every extreme that they name: `expert_ids`: each token's expert, 0 to 255; in every block of 256 tokens one expert, the same in all blocks, is chosen by 2 + 1 or more tokens at positions that differ from block to block. `slots`: the slot of a token is the number of earlier tokens of its block of 256 that chose the same expert, if that is below 2, else -1; so at most 2 tokens of one block reach one expert, and one expert receives exactly 2 from every block.
All inputs are finite; a program needn't handle non-finite values.
Results may differ from the reference program's by a relative error of at most 0.0037.
Values may be sent and summed in bfloat16 or wider, within the bound.
No kernel may reach another device: no remote copies, remote signals or barrier semaphores. Data moves between devices by JAX's collectives and lax.ppermute only.
A program may use at most 64 MiB of HBM per device.

```python
import jax
import jax.numpy as jnp
from jax import lax

D = 768
FF = 3072
TOK_DEV = 256
EXPERTS = 256
CAP = 2
TOKENS = 65536


def routing_pair(key):
    blocks = TOKENS // TOK_DEV
    first, second, third = jax.random.split(jax.random.fold_in(key, 7), 3)
    chosen = jax.random.randint(first, (blocks, TOK_DEV), 0, EXPERTS).astype(jnp.int32)
    popular = jax.random.randint(second, (), 0, EXPERTS).astype(jnp.int32)
    block_keys = jax.random.split(third, blocks)
    orders = jax.vmap(lambda k: jax.random.permutation(k, TOK_DEV))(block_keys)
    inverse = jnp.argsort(orders, axis=1, stable=True)
    forced = inverse < CAP + 1
    chosen = jnp.where(forced, popular, chosen).astype(jnp.int32)
    positions = jnp.arange(TOK_DEV, dtype=jnp.int32)
    earlier_than = positions[None, :] < positions[:, None]

    def ranks(block_ids):
        same = block_ids[:, None] == block_ids[None, :]
        count = jnp.sum((same & earlier_than).astype(jnp.int32), axis=1)
        return jnp.where(count < CAP, count, -1).astype(jnp.int32)
    slot_values = lax.map(ranks, chosen)
    return (chosen.reshape(TOKENS), slot_values.reshape(TOKENS))


def draw_expert_ids(key, part):
    return routing_pair(key)[0]


def draw_slots(key, part):
    return routing_pair(key)[1]


def level_of(key, shape, pieces, least, top_value):
    loudness = 1.0
    for axis_at, parts in pieces:
        heights = jax.random.uniform(jax.random.fold_in(jax.random.fold_in(key, 6), axis_at), (parts,), jnp.float32, least / len(pieces), top_value / len(pieces))
        loudness = loudness * jnp.repeat(jnp.exp(heights), shape[axis_at] // parts).reshape((-1,) + (1,) * (len(shape) - 1 - axis_at))
    return loudness


def noise(stream_key, dims, deviation, most, shards=(), kind=jnp.bfloat16):
    values = deviation * jax.random.normal(stream_key, dims, jnp.float32)
    if shards:
        values = values * level_of(stream_key, dims, shards, -0.22, 0.18)
    return jnp.clip(values, -most, most).astype(kind)


def setup_inputs(seed: int = 0) -> dict:
    key_list = jax.random.split(jax.random.key(seed), 8)
    tokens = noise(key_list[0], (TOKENS, D), 1.0, 6.0, ((0, 256),))
    norm_gain = jnp.clip(1.0 + 0.15 * jax.random.normal(key_list[1], (D,), jnp.float32), 0.25, 1.75)
    gates = jnp.clip(0.25 + 0.75 * jax.random.uniform(key_list[2], (TOKENS,), jnp.float32) ** level_of(key_list[2], (TOKENS,), ((0, 256),), -0.2, 0.2), 0.25, 1.0)
    expert_ids = draw_expert_ids(jax.random.fold_in(key_list[7], 71), 0)
    slots = draw_slots(jax.random.fold_in(key_list[7], 71), 0)
    w_in = noise(key_list[5], (EXPERTS, D, FF), D ** -0.5, 0.21875, ((0, 256),))
    w_out = noise(key_list[6], (EXPERTS, D, FF), FF ** -0.5, 0.109375, ((0, 256),))
    return {"tokens": tokens, "norm_gain": norm_gain, "gates": gates, "expert_ids": expert_ids, "slots": slots, "w_in": w_in, "w_out": w_out}


def slot_mask(expert_ids, slots):
    index = expert_ids * CAP + slots
    columns = jnp.arange(EXPERTS * CAP, dtype=jnp.int32)
    valid = slots >= 0
    return ((index[:, None] == columns[None, :]) & valid[:, None]).astype(jnp.bfloat16)

def normalize(tokens, norm_gain):
    values = tokens.astype(jnp.float32)
    square = lax.optimization_barrier(jnp.mean(values * values, axis=-1, keepdims=True))
    return (values * lax.rsqrt(square + 1e-06) * norm_gain[None, :]).astype(jnp.bfloat16)

def reference(tokens, norm_gain, gates, expert_ids, slots, w_in, w_out):
    blocks = TOKENS // TOK_DEV
    tok_blocks = tokens.reshape(blocks, TOK_DEV, D)
    id_blocks = expert_ids.reshape(blocks, TOK_DEV)
    slot_blocks = slots.reshape(blocks, TOK_DEV)
    gate_blocks = gates.reshape(blocks, TOK_DEV)

    def prepare(items):
        block_tok, block_ids, block_slots = items
        normed = normalize(block_tok, norm_gain)
        masked = slot_mask(block_ids, block_slots)
        filled = jnp.dot(masked.T, normed, preferred_element_type=jnp.float32)
        return filled.astype(jnp.bfloat16).reshape(EXPERTS, CAP, D)
    buffer = lax.map(prepare, (tok_blocks, id_blocks, slot_blocks))

    def run_expert(items):
        rows, weight_in, weight_out = items
        flat = rows.reshape(blocks * CAP, D)
        hidden = jnp.maximum(jnp.dot(flat, weight_in, preferred_element_type=jnp.float32), 0.0).astype(jnp.bfloat16)
        result = jnp.dot(hidden, weight_out.T, preferred_element_type=jnp.float32)
        return result.astype(jnp.bfloat16).reshape(blocks, CAP, D)
    expert_out = lax.map(run_expert, (jnp.transpose(buffer, (1, 0, 2, 3)), w_in, w_out))
    expert_out = jnp.transpose(expert_out, (1, 0, 2, 3))

    def finish(items):
        block_tok, block_ids, block_slots, block_gate, block_out = items
        masked = slot_mask(block_ids, block_slots)
        picked = jnp.dot(masked, block_out.reshape(EXPERTS * CAP, D), preferred_element_type=jnp.float32)
        return (block_tok.astype(jnp.float32) + block_gate[:, None] * picked).astype(jnp.bfloat16)
    mixed = lax.map(finish, (tok_blocks, id_blocks, slot_blocks, gate_blocks, expert_out))
    return mixed.reshape(TOKENS, D)
```

```python
import jax
import jax.numpy as jnp
from jax import lax
from jax.experimental import pallas as pl
from jax.experimental.pallas import tpu as pltpu
from jax.sharding import PartitionSpec as P

AXES = ("expert", "tensor")
CAP = 2
VMEM = pl.BlockSpec(memory_space=pltpu.VMEM)
HBM = pl.BlockSpec(memory_space=pltpu.HBM)
MIB = 2**20


def slot_index(ids_ref, slots_ref):
    slots = slots_ref[...]
    return jnp.where(slots >= 0, ids_ref[...] * CAP + slots, -1)


def dispatch_kernel(
    tokens_hbm,
    gain_hbm,
    gates_hbm,
    ids_hbm,
    slots_hbm,
    w_in_hbm,
    sent_ref,
    tokens_ref,
    gates_ref,
    ids_ref,
    slots_ref,
    w_in_ref,
    gain_ref,
    sems,
):
    pairs = (
        (tokens_hbm, tokens_ref),
        (ids_hbm, ids_ref),
        (slots_hbm, slots_ref),
        (gain_hbm, gain_ref),
        (gates_hbm, gates_ref),
        (w_in_hbm, w_in_ref),
    )
    copies = [pltpu.make_async_copy(a, b, sems.at[i]) for i, (a, b) in enumerate(pairs)]
    for copy in copies:
        copy.start()
    for copy in copies[:5]:
        copy.wait()
    count, _, width = sent_ref.shape
    tok_dev = tokens_ref.shape[0]
    values = tokens_ref[...].astype(jnp.float32)
    square = jnp.mean(values * values, axis=-1, keepdims=True)
    normed = values * lax.rsqrt(square + 1e-06) * gain_ref[...][None, :]
    rows = lax.broadcasted_iota(jnp.int32, (count * CAP, tok_dev), 0)
    masked = (rows == slot_index(ids_ref, slots_ref)[None, :]).astype(jnp.float32)
    buffer = jnp.dot(
        masked.astype(jnp.bfloat16),
        normed.astype(jnp.bfloat16),
        preferred_element_type=jnp.float32,
    )
    sent_ref[...] = buffer.astype(jnp.bfloat16).reshape(count, CAP, width)
    copies[5].wait()


def in_hbm(array):
    return pltpu.with_memory_space_constraint(array, pltpu.HBM)


def dispatch(tokens, norm_gain, gates, expert_ids, slots, w_in, experts):
    tok_dev, width = tokens.shape
    return pl.pallas_call(
        dispatch_kernel,
        out_shape=(
            pltpu.VMEM((experts, CAP, width), jnp.bfloat16),
            *(pltpu.VMEM(a.shape, a.dtype) for a in (tokens, gates, expert_ids, slots, w_in)),
        ),
        in_specs=[HBM] * 6,
        out_specs=(VMEM,) * 6,
        scratch_shapes=[pltpu.VMEM(norm_gain.shape, jnp.float32), pltpu.SemaphoreType.DMA((6,))],
        compiler_params=pltpu.CompilerParams(vmem_limit_bytes=8 * MIB),
        cost_estimate=pl.CostEstimate(
            flops=2 * experts * CAP * tok_dev * width,
            bytes_accessed=2 * tok_dev * width + 2 * w_in.size,
            transcendentals=tok_dev,
        ),
        name="dispatch",
    )(*(in_hbm(a) for a in (tokens, norm_gain, gates, expert_ids, slots, w_in)))


def expert_kernel(rows_ref, w_in_ref, w_out_hbm, out_ref, hidden_ref, w_out_ref, sem):
    copy = pltpu.make_async_copy(w_out_hbm, w_out_ref, sem)
    copy.start()
    blocks, _, width = rows_ref.shape
    ff = w_in_ref.shape[-1]
    rows = rows_ref[...].reshape(blocks * CAP, width)
    tile = 512
    for at in range(0, ff, tile):
        part = jnp.dot(rows, w_in_ref[0, :, at : at + tile], preferred_element_type=jnp.float32)
        hidden_ref[:, at : at + tile] = jnp.maximum(part, 0.0).astype(jnp.bfloat16)
    copy.wait()
    tile = 256
    for at in range(0, width, tile):
        part = lax.dot_general(
            hidden_ref[...],
            w_out_ref[0, at : at + tile, :],
            (((1,), (1,)), ((), ())),
            preferred_element_type=jnp.float32,
        )
        out_ref[:, :, at : at + tile] = part.astype(jnp.bfloat16).reshape(blocks, CAP, tile)


def run_expert(rows, w_in, w_out):
    blocks, _, width = rows.shape
    ff = w_in.shape[-1]
    return pl.pallas_call(
        expert_kernel,
        out_shape=pltpu.VMEM(rows.shape, jnp.bfloat16),
        in_specs=[VMEM, VMEM, HBM],
        out_specs=VMEM,
        scratch_shapes=[
            pltpu.VMEM((blocks * CAP, ff), jnp.bfloat16),
            pltpu.VMEM(w_out.shape, w_out.dtype),
            pltpu.SemaphoreType.DMA,
        ],
        compiler_params=pltpu.CompilerParams(vmem_limit_bytes=24 * MIB),
        cost_estimate=pl.CostEstimate(
            flops=4 * blocks * CAP * width * ff, bytes_accessed=4 * width * ff, transcendentals=0
        ),
        name="expert_ffn",
    )(rows, w_in, in_hbm(w_out))


def combine_kernel(returned_ref, tokens_ref, gates_ref, ids_ref, slots_ref, mixed_ref):
    experts, _, width = returned_ref.shape
    tok_dev = tokens_ref.shape[0]
    columns = lax.broadcasted_iota(jnp.int32, (tok_dev, experts * CAP), 1)
    masked = (columns == slot_index(ids_ref, slots_ref).reshape(tok_dev, 1)).astype(jnp.float32)
    picked = jnp.dot(
        masked.astype(jnp.bfloat16),
        returned_ref[...].reshape(experts * CAP, width),
        preferred_element_type=jnp.float32,
    )
    gates = gates_ref[...].reshape(tok_dev, 1)
    mixed_ref[...] = (tokens_ref[...].astype(jnp.float32) + gates * picked).astype(jnp.bfloat16)


def combine(returned, tokens, gates, expert_ids, slots):
    experts, _, width = returned.shape
    tok_dev = tokens.shape[0]
    return pl.pallas_call(
        combine_kernel,
        out_shape=jax.ShapeDtypeStruct(tokens.shape, jnp.bfloat16),
        in_specs=[VMEM] * 5,
        out_specs=VMEM,
        compiler_params=pltpu.CompilerParams(vmem_limit_bytes=8 * MIB),
        cost_estimate=pl.CostEstimate(
            flops=2 * experts * CAP * tok_dev * width,
            bytes_accessed=2 * tok_dev * width,
            transcendentals=0,
        ),
        name="combine",
    )(returned, tokens, gates, expert_ids, slots)


def exchange(blocks):
    return lax.all_to_all(blocks, AXES, 0, 0, tiled=True)


def local(tokens, norm_gain, gates, expert_ids, slots, w_in, w_out):
    experts = lax.axis_size("expert") * lax.axis_size("tensor")
    sent, *kept, near_w_in = dispatch(tokens, norm_gain, gates, expert_ids, slots, w_in, experts)
    result = run_expert(exchange(sent), near_w_in, w_out)
    return combine(exchange(result), *kept)


def solution(mesh):
    rows = P(AXES)
    matrix = P(AXES, None)
    weights = P(AXES, None, None)
    return jax.shard_map(
        local,
        mesh=mesh,
        in_specs=(matrix, P(), rows, rows, rows, weights, weights),
        out_specs=matrix,
        check_vma=False,
    )
```

```python
import jax
import jax.numpy as jnp
from jax import lax
from jax.experimental import pallas as pl
from jax.experimental.pallas import tpu as pltpu
from jax.sharding import PartitionSpec as P

AXES = ("expert", "tensor")
CAP = 2
VMEM = pl.BlockSpec(memory_space=pltpu.VMEM)
HBM = pl.BlockSpec(memory_space=pltpu.HBM)
MIB = 2**20


def slot_index(ids_ref, slots_ref):
    slots = slots_ref[...]
    return jnp.where(slots >= 0, ids_ref[...] * CAP + slots, -1)


def dispatch_kernel(
    tokens_hbm,
    gain_hbm,
    gates_hbm,
    ids_hbm,
    slots_hbm,
    w_in_hbm,
    sent_ref,
    tokens_ref,
    gates_ref,
    ids_ref,
    slots_ref,
    w_in_ref,
    gain_ref,
    sems,
):
    pairs = (
        (tokens_hbm, tokens_ref),
        (ids_hbm, ids_ref),
        (slots_hbm, slots_ref),
        (gain_hbm, gain_ref),
        (gates_hbm, gates_ref),
        (w_in_hbm, w_in_ref),
    )
    copies = [pltpu.make_async_copy(a, b, sems.at[i]) for i, (a, b) in enumerate(pairs)]
    for copy in copies:
        copy.start()
    for copy in copies[:5]:
        copy.wait()
    count, _, width = sent_ref.shape
    tok_dev = tokens_ref.shape[0]
    values = tokens_ref[...].astype(jnp.float32)
    square = jnp.mean(values * values, axis=-1, keepdims=True)
    normed = values * lax.rsqrt(square + 1e-06) * gain_ref[...][None, :]
    rows = lax.broadcasted_iota(jnp.int32, (count * CAP, tok_dev), 0)
    masked = (rows == slot_index(ids_ref, slots_ref)[None, :]).astype(jnp.float32)
    buffer = jnp.dot(
        masked.astype(jnp.bfloat16),
        normed.astype(jnp.bfloat16),
        preferred_element_type=jnp.float32,
    )
    sent_ref[...] = buffer.astype(jnp.bfloat16).reshape(count, CAP, width)
    copies[5].wait()


def in_hbm(array):
    return pltpu.with_memory_space_constraint(array, pltpu.HBM)


def dispatch(tokens, norm_gain, gates, expert_ids, slots, w_in, experts):
    tok_dev, width = tokens.shape
    return pl.pallas_call(
        dispatch_kernel,
        out_shape=(
            pltpu.VMEM((experts, CAP, width), jnp.bfloat16),
            *(pltpu.VMEM(a.shape, a.dtype) for a in (tokens, gates, expert_ids, slots, w_in)),
        ),
        in_specs=[HBM] * 6,
        out_specs=(VMEM,) * 6,
        scratch_shapes=[pltpu.VMEM(norm_gain.shape, jnp.float32), pltpu.SemaphoreType.DMA((6,))],
        compiler_params=pltpu.CompilerParams(vmem_limit_bytes=8 * MIB),
        cost_estimate=pl.CostEstimate(
            flops=2 * experts * CAP * tok_dev * width,
            bytes_accessed=2 * tok_dev * width + 2 * w_in.size,
            transcendentals=tok_dev,
        ),
        name="dispatch",
    )(*(in_hbm(a) for a in (tokens, norm_gain, gates, expert_ids, slots, w_in)))


def expert_kernel(rows_ref, w_in_ref, w_out_hbm, out_ref, flat_ref, hidden_ref, w_out_ref, sem):
    copy = pltpu.make_async_copy(w_out_hbm, w_out_ref, sem)
    copy.start()
    blocks, _, width = rows_ref.shape
    ff = w_in_ref.shape[-1]
    flat_ref[...] = rows_ref[...].reshape(blocks * CAP, width)
    tile = ff // 2

    @pl.loop(0, ff // tile)
    def _(step):
        at = pl.multiple_of(step * tile, tile)
        part = jnp.dot(
            flat_ref[...], w_in_ref[0, :, pl.ds(at, tile)], preferred_element_type=jnp.float32
        )
        hidden_ref[:, pl.ds(at, tile)] = jnp.maximum(part, 0.0).astype(jnp.bfloat16)

    copy.wait()
    tile = 256
    for at in range(0, width, tile):
        part = lax.dot_general(
            hidden_ref[...],
            w_out_ref[0, at : at + tile, :],
            (((1,), (1,)), ((), ())),
            preferred_element_type=jnp.float32,
        )
        out_ref[:, :, at : at + tile] = part.astype(jnp.bfloat16).reshape(blocks, CAP, tile)


def run_expert(rows, w_in, w_out):
    blocks, _, width = rows.shape
    ff = w_in.shape[-1]
    return pl.pallas_call(
        expert_kernel,
        out_shape=pltpu.VMEM(rows.shape, jnp.bfloat16),
        in_specs=[VMEM, VMEM, HBM],
        out_specs=VMEM,
        scratch_shapes=[
            pltpu.VMEM((blocks * CAP, width), jnp.bfloat16),
            pltpu.VMEM((blocks * CAP, ff), jnp.bfloat16),
            pltpu.VMEM(w_out.shape, w_out.dtype),
            pltpu.SemaphoreType.DMA,
        ],
        compiler_params=pltpu.CompilerParams(vmem_limit_bytes=24 * MIB),
        cost_estimate=pl.CostEstimate(
            flops=4 * blocks * CAP * width * ff, bytes_accessed=4 * width * ff, transcendentals=0
        ),
        name="expert_ffn",
    )(rows, w_in, in_hbm(w_out))


def combine_kernel(returned_ref, tokens_ref, gates_ref, ids_ref, slots_ref, mixed_ref):
    experts, _, width = returned_ref.shape
    tok_dev = tokens_ref.shape[0]
    columns = lax.broadcasted_iota(jnp.int32, (tok_dev, experts * CAP), 1)
    masked = (columns == slot_index(ids_ref, slots_ref).reshape(tok_dev, 1)).astype(jnp.float32)
    picked = jnp.dot(
        masked.astype(jnp.bfloat16),
        returned_ref[...].reshape(experts * CAP, width),
        preferred_element_type=jnp.float32,
    )
    gates = gates_ref[...].reshape(tok_dev, 1)
    mixed_ref[...] = (tokens_ref[...].astype(jnp.float32) + gates * picked).astype(jnp.bfloat16)


def combine(returned, tokens, gates, expert_ids, slots):
    experts, _, width = returned.shape
    tok_dev = tokens.shape[0]
    return pl.pallas_call(
        combine_kernel,
        out_shape=jax.ShapeDtypeStruct(tokens.shape, jnp.bfloat16),
        in_specs=[VMEM] * 5,
        out_specs=VMEM,
        compiler_params=pltpu.CompilerParams(vmem_limit_bytes=8 * MIB),
        cost_estimate=pl.CostEstimate(
            flops=2 * experts * CAP * tok_dev * width,
            bytes_accessed=2 * tok_dev * width,
            transcendentals=0,
        ),
        name="combine",
    )(returned, tokens, gates, expert_ids, slots)


def exchange(blocks):
    return lax.all_to_all(blocks, AXES, 0, 0, tiled=True)


def local(tokens, norm_gain, gates, expert_ids, slots, w_in, w_out):
    experts = lax.axis_size("expert") * lax.axis_size("tensor")
    sent, *kept, near_w_in = dispatch(tokens, norm_gain, gates, expert_ids, slots, w_in, experts)
    result = run_expert(exchange(sent), near_w_in, w_out)
    return combine(exchange(result), *kept)


def solution(mesh):
    rows = P(AXES)
    matrix = P(AXES, None)
    weights = P(AXES, None, None)
    return jax.shard_map(
        local,
        mesh=mesh,
        in_specs=(matrix, P(), rows, rows, rows, weights, weights),
        out_specs=matrix,
        check_vma=False,
    )
```

```python
import jax
import jax.numpy as jnp
from jax import lax
from jax.experimental import pallas as pl
from jax.experimental.pallas import tpu as pltpu
from jax.sharding import PartitionSpec as P

AXES = ("expert", "tensor")
CAP = 2
HALVES = 2
RETURN_ORDER = (0, 4, 5, 6, 7, 1, 2, 3)
VMEM = pl.BlockSpec(memory_space=pltpu.VMEM)
HBM = pl.BlockSpec(memory_space=pltpu.HBM)
MIB = 2**20


def slot_index(owners, slots_ref):
    slots = slots_ref[...]
    return jnp.where(slots >= 0, owners * CAP + slots, -1)


def return_position(ids, experts):
    span = experts // len(RETURN_ORDER)
    shift = jnp.zeros_like(ids)
    for at, group in enumerate(RETURN_ORDER):
        inside = (ids >= group * span) & (ids < (group + 1) * span)
        shift = jnp.where(inside, (at - group) * span, shift)
    return ids + shift


def return_group(experts):
    span = experts // len(RETURN_ORDER)
    return [group * span + i for group in RETURN_ORDER for i in range(span)]


def dispatch_kernel(
    tokens_hbm,
    gain_hbm,
    gates_hbm,
    ids_hbm,
    slots_hbm,
    w_in_hbm,
    sent_ref,
    tokens_ref,
    gates_ref,
    ids_ref,
    slots_ref,
    w_in_ref,
    gain_ref,
    sems,
):
    pairs = (
        (tokens_hbm, tokens_ref),
        (ids_hbm, ids_ref),
        (slots_hbm, slots_ref),
        (gain_hbm, gain_ref),
        (gates_hbm, gates_ref),
        (w_in_hbm.at[0, :, : w_in_ref.shape[-1]], w_in_ref.at[0]),
    )
    copies = [pltpu.make_async_copy(a, b, sems.at[i]) for i, (a, b) in enumerate(pairs)]
    for copy in copies:
        copy.start()
    for copy in copies[:5]:
        copy.wait()
    count, _, width = sent_ref.shape
    tok_dev = tokens_ref.shape[0]
    values = tokens_ref[...].astype(jnp.float32)
    square = jnp.mean(values * values, axis=-1, keepdims=True)
    normed = values * lax.rsqrt(square + 1e-06) * gain_ref[...][None, :]
    rows = lax.broadcasted_iota(jnp.int32, (count * CAP, tok_dev), 0)
    masked = (rows == slot_index(ids_ref[...], slots_ref)[None, :]).astype(jnp.float32)
    buffer = jnp.dot(
        masked.astype(jnp.bfloat16),
        normed.astype(jnp.bfloat16),
        preferred_element_type=jnp.float32,
    )
    sent_ref[...] = buffer.astype(jnp.bfloat16).reshape(count, CAP, width)
    copies[5].wait()


def in_hbm(array):
    return pltpu.with_memory_space_constraint(array, pltpu.HBM)


def dispatch(tokens, norm_gain, gates, expert_ids, slots, w_in, experts):
    tok_dev, width = tokens.shape
    return pl.pallas_call(
        dispatch_kernel,
        out_shape=(
            pltpu.VMEM((experts, CAP, width), jnp.bfloat16),
            *(pltpu.VMEM(a.shape, a.dtype) for a in (tokens, gates, expert_ids, slots)),
            pltpu.VMEM((HALVES, width, w_in.shape[-1] // HALVES), w_in.dtype),
        ),
        in_specs=[HBM] * 6,
        out_specs=(VMEM,) * 6,
        scratch_shapes=[pltpu.VMEM(norm_gain.shape, jnp.float32), pltpu.SemaphoreType.DMA((6,))],
        compiler_params=pltpu.CompilerParams(vmem_limit_bytes=8 * MIB),
        cost_estimate=pl.CostEstimate(
            flops=2 * experts * CAP * tok_dev * width,
            bytes_accessed=2 * tok_dev * width + 2 * w_in.size,
            transcendentals=tok_dev,
        ),
        name="dispatch",
    )(*(in_hbm(a) for a in (tokens, norm_gain, gates, expert_ids, slots, w_in)))


def expert_kernel(
    rows_ref, _, w_in_hbm, w_out_hbm, out_ref, w_in_ref, flat_ref, hidden_ref, w_out_ref, sems
):
    blocks, _, width = rows_ref.shape
    tile = w_in_ref.shape[-1]
    out_tile = 256
    outs = range(0, width, out_tile)
    late = [
        pltpu.make_async_copy(
            w_in_hbm.at[0, :, half * tile : (half + 1) * tile], w_in_ref.at[half], sems.at[half]
        )
        for half in range(1, HALVES)
    ]
    lasts = [
        pltpu.make_async_copy(
            w_out_hbm.at[0, at : at + out_tile], w_out_ref.at[at : at + out_tile], sems.at[HALVES + i]
        )
        for i, at in enumerate(outs)
    ]
    for copy in late + lasts:
        copy.start()
    span = blocks // len(RETURN_ORDER)
    for at, group in enumerate(RETURN_ORDER):
        rows = rows_ref[group * span : (group + 1) * span].reshape(span * CAP, width)
        flat_ref[at * span * CAP : (at + 1) * span * CAP] = rows

    @pl.loop(0, HALVES)
    def _(step):
        for half in range(1, HALVES):

            @pl.when(step == half)
            def _():
                late[half - 1].wait()

        part = jnp.dot(flat_ref[...], w_in_ref[step], preferred_element_type=jnp.float32)
        at = pl.multiple_of(step * tile, tile)
        hidden_ref[:, pl.ds(at, tile)] = jnp.maximum(part, 0.0).astype(jnp.bfloat16)

    for copy in lasts:
        copy.wait()
    for at in outs:
        part = lax.dot_general(
            hidden_ref[...],
            w_out_ref[at : at + out_tile],
            (((1,), (1,)), ((), ())),
            preferred_element_type=jnp.float32,
        )
        out_ref[:, :, at : at + out_tile] = part.astype(jnp.bfloat16).reshape(blocks, CAP, out_tile)


def run_expert(rows, near_w_in, w_in, w_out):
    blocks, _, width = rows.shape
    ff = w_in.shape[-1]
    return pl.pallas_call(
        expert_kernel,
        out_shape=(
            pltpu.VMEM(rows.shape, jnp.bfloat16),
            pltpu.VMEM(near_w_in.shape, near_w_in.dtype),
        ),
        in_specs=[VMEM, VMEM, HBM, HBM],
        out_specs=(VMEM, VMEM),
        input_output_aliases={1: 1},
        scratch_shapes=[
            pltpu.VMEM((blocks * CAP, width), jnp.bfloat16),
            pltpu.VMEM((blocks * CAP, ff), jnp.bfloat16),
            pltpu.VMEM((width, ff), w_out.dtype),
            pltpu.SemaphoreType.DMA((HALVES + 3,)),
        ],
        compiler_params=pltpu.CompilerParams(vmem_limit_bytes=24 * MIB),
        cost_estimate=pl.CostEstimate(
            flops=4 * blocks * CAP * width * ff, bytes_accessed=4 * width * ff, transcendentals=0
        ),
        name="expert_ffn",
    )(rows, near_w_in, in_hbm(w_in), in_hbm(w_out))[0]


def combine_kernel(
    returned_ref, tokens_ref, gates_ref, ids_ref, slots_ref, mixed_hbm, mixed_ref, sems
):
    experts, _, width = returned_ref.shape
    tok_dev = tokens_ref.shape[0]
    owners = return_position(ids_ref[...], experts)
    index = slot_index(owners, slots_ref).reshape(tok_dev, 1)
    gates = gates_ref[...].reshape(tok_dev, 1)
    returned = returned_ref[...].reshape(experts * CAP, width)
    part = tok_dev // 2
    columns = lax.broadcasted_iota(jnp.int32, (part, experts * CAP), 1)
    copies = []
    for at in range(0, tok_dev, part):
        rows = slice(at, at + part)
        masked = (columns == index[rows]).astype(jnp.float32).astype(jnp.bfloat16)
        picked = jnp.dot(masked, returned, preferred_element_type=jnp.float32)
        mixed = tokens_ref[rows].astype(jnp.float32) + gates[rows] * picked
        mixed_ref[rows] = mixed.astype(jnp.bfloat16)
        copy = pltpu.make_async_copy(mixed_ref.at[rows], mixed_hbm.at[rows], sems.at[at // part])
        copy.start()
        copies.append(copy)
    for copy in copies:
        copy.wait()


def combine(returned, tokens, gates, expert_ids, slots):
    experts, _, width = returned.shape
    tok_dev = tokens.shape[0]
    return pl.pallas_call(
        combine_kernel,
        out_shape=jax.ShapeDtypeStruct(tokens.shape, jnp.bfloat16),
        in_specs=[VMEM] * 5,
        out_specs=HBM,
        scratch_shapes=[
            pltpu.VMEM(tokens.shape, jnp.bfloat16),
            pltpu.SemaphoreType.DMA((2,)),
        ],
        compiler_params=pltpu.CompilerParams(vmem_limit_bytes=8 * MIB),
        cost_estimate=pl.CostEstimate(
            flops=2 * experts * CAP * tok_dev * width,
            bytes_accessed=2 * tok_dev * width,
            transcendentals=0,
        ),
        name="combine",
    )(returned, tokens, gates, expert_ids, slots)


def exchange(blocks, groups=None):
    return lax.all_to_all(blocks, AXES, 0, 0, tiled=True, axis_index_groups=groups)


def local(tokens, norm_gain, gates, expert_ids, slots, w_in, w_out):
    experts = lax.axis_size("expert") * lax.axis_size("tensor")
    sent, *kept, near_w_in = dispatch(tokens, norm_gain, gates, expert_ids, slots, w_in, experts)
    result = run_expert(exchange(sent), near_w_in, w_in, w_out)
    return combine(exchange(result, [return_group(experts)]), *kept)


def solution(mesh):
    rows = P(AXES)
    matrix = P(AXES, None)
    weights = P(AXES, None, None)
    return jax.shard_map(
        local,
        mesh=mesh,
        in_specs=(matrix, P(), rows, rows, rows, weights, weights),
        out_specs=matrix,
        check_vma=False,
    )
```

```python
import jax
import jax.numpy as jnp
from jax import lax
from jax.experimental import pallas as pl
from jax.experimental.pallas import tpu as pltpu
from jax.sharding import PartitionSpec as P

AXES = ("expert", "tensor")
CAP = 2
HALVES = 2
DISPATCH_ORDER = (0, 1, 4, 2, 6, 5, 7, 3)
RETURN_ORDER = (0, 4, 5, 6, 7, 1, 2, 3)
VMEM = pl.BlockSpec(memory_space=pltpu.VMEM)
HBM = pl.BlockSpec(memory_space=pltpu.HBM)
MIB = 2**20


def slot_index(owners, slots_ref):
    slots = slots_ref[...]
    return jnp.where(slots >= 0, owners * CAP + slots, -1)


def position_of(ids, order, experts):
    span = experts // len(order)
    shift = jnp.zeros_like(ids)
    for at, group in enumerate(order):
        inside = (ids >= group * span) & (ids < (group + 1) * span)
        shift = jnp.where(inside, (at - group) * span, shift)
    return ids + shift


def members(order, experts):
    span = experts // len(order)
    return [group * span + i for group in order for i in range(span)]


def dispatch_kernel(
    tokens_hbm,
    gain_hbm,
    gates_hbm,
    ids_hbm,
    slots_hbm,
    w_in_hbm,
    sent_ref,
    tokens_ref,
    gates_ref,
    ids_ref,
    slots_ref,
    w_in_ref,
    gain_ref,
    sems,
):
    pairs = (
        (tokens_hbm, tokens_ref),
        (ids_hbm, ids_ref),
        (slots_hbm, slots_ref),
        (gain_hbm, gain_ref),
        (gates_hbm, gates_ref),
        (w_in_hbm.at[0, :, : w_in_ref.shape[-1]], w_in_ref.at[0]),
    )
    copies = [pltpu.make_async_copy(a, b, sems.at[i]) for i, (a, b) in enumerate(pairs)]
    for copy in copies:
        copy.start()
    for copy in copies[:5]:
        copy.wait()
    count, _, width = sent_ref.shape
    tok_dev = tokens_ref.shape[0]
    values = tokens_ref[...].astype(jnp.float32)
    square = jnp.mean(values * values, axis=-1, keepdims=True)
    normed = values * lax.rsqrt(square + 1e-06) * gain_ref[...][None, :]
    rows = lax.broadcasted_iota(jnp.int32, (count * CAP, tok_dev), 0)
    owners = position_of(ids_ref[...], DISPATCH_ORDER, count)
    masked = (rows == slot_index(owners, slots_ref)[None, :]).astype(jnp.float32)
    buffer = jnp.dot(
        masked.astype(jnp.bfloat16),
        normed.astype(jnp.bfloat16),
        preferred_element_type=jnp.float32,
    )
    sent_ref[...] = buffer.astype(jnp.bfloat16).reshape(count, CAP, width)
    copies[5].wait()


def in_hbm(array):
    return pltpu.with_memory_space_constraint(array, pltpu.HBM)


def dispatch(tokens, norm_gain, gates, expert_ids, slots, w_in, experts):
    tok_dev, width = tokens.shape
    return pl.pallas_call(
        dispatch_kernel,
        out_shape=(
            pltpu.VMEM((experts, CAP, width), jnp.bfloat16),
            *(pltpu.VMEM(a.shape, a.dtype) for a in (tokens, gates, expert_ids, slots)),
            pltpu.VMEM((HALVES, width, w_in.shape[-1] // HALVES), w_in.dtype),
        ),
        in_specs=[HBM] * 6,
        out_specs=(VMEM,) * 6,
        scratch_shapes=[pltpu.VMEM(norm_gain.shape, jnp.float32), pltpu.SemaphoreType.DMA((6,))],
        compiler_params=pltpu.CompilerParams(vmem_limit_bytes=8 * MIB),
        cost_estimate=pl.CostEstimate(
            flops=2 * experts * CAP * tok_dev * width,
            bytes_accessed=2 * tok_dev * width + 2 * w_in.size,
            transcendentals=tok_dev,
        ),
        name="dispatch",
    )(*(in_hbm(a) for a in (tokens, norm_gain, gates, expert_ids, slots, w_in)))


def expert_kernel(
    rows_ref, _, w_in_hbm, w_out_hbm, out_ref, w_in_ref, flat_ref, hidden_ref, w_out_ref, sems
):
    blocks, _, width = rows_ref.shape
    tile = w_in_ref.shape[-1]
    out_tile = 256
    outs = range(0, width, out_tile)
    late = [
        pltpu.make_async_copy(
            w_in_hbm.at[0, :, half * tile : (half + 1) * tile], w_in_ref.at[half], sems.at[half]
        )
        for half in range(1, HALVES)
    ]
    lasts = [
        pltpu.make_async_copy(
            w_out_hbm.at[0, at : at + out_tile], w_out_ref.at[at : at + out_tile], sems.at[HALVES + i]
        )
        for i, at in enumerate(outs)
    ]
    for copy in late + lasts:
        copy.start()
    span = blocks // len(RETURN_ORDER)
    for at, group in enumerate(RETURN_ORDER):
        came = DISPATCH_ORDER.index(group) * span
        rows = rows_ref[came : came + span].reshape(span * CAP, width)
        flat_ref[at * span * CAP : (at + 1) * span * CAP] = rows

    @pl.loop(0, HALVES)
    def _(step):
        for half in range(1, HALVES):

            @pl.when(step == half)
            def _():
                late[half - 1].wait()

        part = jnp.dot(flat_ref[...], w_in_ref[step], preferred_element_type=jnp.float32)
        at = pl.multiple_of(step * tile, tile)
        hidden_ref[:, pl.ds(at, tile)] = jnp.maximum(part, 0.0).astype(jnp.bfloat16)

    for copy in lasts:
        copy.wait()
    for at in outs:
        part = lax.dot_general(
            hidden_ref[...],
            w_out_ref[at : at + out_tile],
            (((1,), (1,)), ((), ())),
            preferred_element_type=jnp.float32,
        )
        out_ref[:, :, at : at + out_tile] = part.astype(jnp.bfloat16).reshape(blocks, CAP, out_tile)


def run_expert(rows, near_w_in, w_in, w_out):
    blocks, _, width = rows.shape
    ff = w_in.shape[-1]
    return pl.pallas_call(
        expert_kernel,
        out_shape=(
            pltpu.VMEM(rows.shape, jnp.bfloat16),
            pltpu.VMEM(near_w_in.shape, near_w_in.dtype),
        ),
        in_specs=[VMEM, VMEM, HBM, HBM],
        out_specs=(VMEM, VMEM),
        input_output_aliases={1: 1},
        scratch_shapes=[
            pltpu.VMEM((blocks * CAP, width), jnp.bfloat16),
            pltpu.VMEM((blocks * CAP, ff), jnp.bfloat16),
            pltpu.VMEM((width, ff), w_out.dtype),
            pltpu.SemaphoreType.DMA((HALVES + 3,)),
        ],
        compiler_params=pltpu.CompilerParams(vmem_limit_bytes=24 * MIB),
        cost_estimate=pl.CostEstimate(
            flops=4 * blocks * CAP * width * ff, bytes_accessed=4 * width * ff, transcendentals=0
        ),
        name="expert_ffn",
    )(rows, near_w_in, in_hbm(w_in), in_hbm(w_out))[0]


def combine_kernel(
    returned_ref, tokens_ref, gates_ref, ids_ref, slots_ref, mixed_hbm, mixed_ref, sems
):
    experts, _, width = returned_ref.shape
    tok_dev = tokens_ref.shape[0]
    owners = position_of(ids_ref[...], RETURN_ORDER, experts)
    index = slot_index(owners, slots_ref).reshape(tok_dev, 1)
    gates = gates_ref[...].reshape(tok_dev, 1)
    returned = returned_ref[...].reshape(experts * CAP, width)
    part = tok_dev // 2
    columns = lax.broadcasted_iota(jnp.int32, (part, experts * CAP), 1)
    copies = []
    for at in range(0, tok_dev, part):
        rows = slice(at, at + part)
        masked = (columns == index[rows]).astype(jnp.float32).astype(jnp.bfloat16)
        picked = jnp.dot(masked, returned, preferred_element_type=jnp.float32)
        mixed = tokens_ref[rows].astype(jnp.float32) + gates[rows] * picked
        mixed_ref[rows] = mixed.astype(jnp.bfloat16)
        copy = pltpu.make_async_copy(mixed_ref.at[rows], mixed_hbm.at[rows], sems.at[at // part])
        copy.start()
        copies.append(copy)
    for copy in copies:
        copy.wait()


def combine(returned, tokens, gates, expert_ids, slots):
    experts, _, width = returned.shape
    tok_dev = tokens.shape[0]
    return pl.pallas_call(
        combine_kernel,
        out_shape=jax.ShapeDtypeStruct(tokens.shape, jnp.bfloat16),
        in_specs=[VMEM] * 5,
        out_specs=HBM,
        scratch_shapes=[
            pltpu.VMEM(tokens.shape, jnp.bfloat16),
            pltpu.SemaphoreType.DMA((2,)),
        ],
        compiler_params=pltpu.CompilerParams(vmem_limit_bytes=8 * MIB),
        cost_estimate=pl.CostEstimate(
            flops=2 * experts * CAP * tok_dev * width,
            bytes_accessed=2 * tok_dev * width,
            transcendentals=0,
        ),
        name="combine",
    )(returned, tokens, gates, expert_ids, slots)


def exchange(blocks, order):
    groups = [members(order, blocks.shape[0])]
    return lax.all_to_all(blocks, AXES, 0, 0, tiled=True, axis_index_groups=groups)


def local(tokens, norm_gain, gates, expert_ids, slots, w_in, w_out):
    experts = lax.axis_size("expert") * lax.axis_size("tensor")
    sent, *kept, near_w_in = dispatch(tokens, norm_gain, gates, expert_ids, slots, w_in, experts)
    result = run_expert(exchange(sent, DISPATCH_ORDER), near_w_in, w_in, w_out)
    return combine(exchange(result, RETURN_ORDER), *kept)


def solution(mesh):
    rows = P(AXES)
    matrix = P(AXES, None)
    weights = P(AXES, None, None)
    return jax.shard_map(
        local,
        mesh=mesh,
        in_specs=(matrix, P(), rows, rows, rows, weights, weights),
        out_specs=matrix,
        check_vma=False,
    )
```

```python
import jax
import jax.numpy as jnp
from jax import lax
from jax.experimental import pallas as pl
from jax.experimental.pallas import tpu as pltpu
from jax.sharding import PartitionSpec as P

AXES = ("expert", "tensor")
CAP = 2
HALVES = 2
LATE_PARTS = 1
DISPATCH_ORDER = (0, 1, 4, 2, 6, 5, 7, 3)
RETURN_ORDER = (0, 4, 5, 6, 7, 1, 2, 3)
VMEM = pl.BlockSpec(memory_space=pltpu.VMEM)
HBM = pl.BlockSpec(memory_space=pltpu.HBM)
MIB = 2**20


def slot_index(owners, slots_ref):
    slots = slots_ref[...]
    return jnp.where(slots >= 0, owners * CAP + slots, -1)


def position_of(ids, order, experts):
    span = experts // len(order)
    shift = jnp.zeros_like(ids)
    for at, group in enumerate(order):
        inside = (ids >= group * span) & (ids < (group + 1) * span)
        shift = jnp.where(inside, (at - group) * span, shift)
    return ids + shift


def members(order, experts):
    span = experts // len(order)
    return [group * span + i for group in order for i in range(span)]


def dispatch_kernel(
    tokens_hbm,
    gain_hbm,
    gates_hbm,
    ids_hbm,
    slots_hbm,
    w_in_hbm,
    sent_ref,
    tokens_ref,
    gates_ref,
    ids_ref,
    slots_ref,
    w_in_ref,
    gain_ref,
    sems,
):
    pairs = (
        (tokens_hbm, tokens_ref),
        (ids_hbm, ids_ref),
        (slots_hbm, slots_ref),
        (gain_hbm, gain_ref),
        (gates_hbm, gates_ref),
        (w_in_hbm.at[0, :, : w_in_ref.shape[-1]], w_in_ref.at[0]),
    )
    copies = [pltpu.make_async_copy(a, b, sems.at[i]) for i, (a, b) in enumerate(pairs)]
    for copy in copies:
        copy.start()
    for copy in copies[:5]:
        copy.wait()
    count, _, width = sent_ref.shape
    tok_dev = tokens_ref.shape[0]
    values = tokens_ref[...].astype(jnp.float32)
    square = jnp.mean(values * values, axis=-1, keepdims=True)
    normed = values * lax.rsqrt(square + 1e-06) * gain_ref[...][None, :]
    rows = lax.broadcasted_iota(jnp.int32, (count * CAP, tok_dev), 0)
    owners = position_of(ids_ref[...], DISPATCH_ORDER, count)
    masked = (rows == slot_index(owners, slots_ref)[None, :]).astype(jnp.float32)
    buffer = jnp.dot(
        masked.astype(jnp.bfloat16),
        normed.astype(jnp.bfloat16),
        preferred_element_type=jnp.float32,
    )
    sent_ref[...] = buffer.astype(jnp.bfloat16).reshape(count, CAP, width)
    copies[5].wait()


def in_hbm(array):
    return pltpu.with_memory_space_constraint(array, pltpu.HBM)


def dispatch(tokens, norm_gain, gates, expert_ids, slots, w_in, experts):
    tok_dev, width = tokens.shape
    return pl.pallas_call(
        dispatch_kernel,
        out_shape=(
            pltpu.VMEM((experts, CAP, width), jnp.bfloat16),
            *(pltpu.VMEM(a.shape, a.dtype) for a in (tokens, gates, expert_ids, slots)),
            pltpu.VMEM((HALVES, width, w_in.shape[-1] // HALVES), w_in.dtype),
        ),
        in_specs=[HBM] * 6,
        out_specs=(VMEM,) * 6,
        scratch_shapes=[pltpu.VMEM(norm_gain.shape, jnp.float32), pltpu.SemaphoreType.DMA((6,))],
        compiler_params=pltpu.CompilerParams(vmem_limit_bytes=8 * MIB),
        cost_estimate=pl.CostEstimate(
            flops=2 * experts * CAP * tok_dev * width,
            bytes_accessed=2 * tok_dev * width + 2 * w_in.size,
            transcendentals=tok_dev,
        ),
        name="dispatch",
    )(*(in_hbm(a) for a in (tokens, norm_gain, gates, expert_ids, slots, w_in)))


def expert_kernel(
    rows_ref, _, w_in_hbm, w_out_hbm, out_ref, w_in_ref, flat_ref, hidden_ref, w_out_ref, sems
):
    blocks, _, width = rows_ref.shape
    tile = w_in_ref.shape[-1]
    out_tile = 256
    outs = range(0, width, out_tile)
    part_rows = width // LATE_PARTS
    late = [
        pltpu.make_async_copy(
            w_in_hbm.at[0, at : at + part_rows, tile:],
            w_in_ref.at[1, at : at + part_rows],
            sems.at[at // part_rows],
        )
        for at in range(0, width, part_rows)
    ]
    lasts = [pltpu.make_async_copy(w_out_hbm.at[0], w_out_ref, sems.at[LATE_PARTS])]
    for copy in late + lasts:
        copy.start()
    span = blocks // len(RETURN_ORDER)
    for at, group in enumerate(RETURN_ORDER):
        came = DISPATCH_ORDER.index(group) * span
        rows = rows_ref[came : came + span].reshape(span * CAP, width)
        flat_ref[at * span * CAP : (at + 1) * span * CAP] = rows

    @pl.loop(0, HALVES)
    def _(step):
        @pl.when(step == 1)
        def _():
            for copy in late:
                copy.wait()

        part = jnp.dot(flat_ref[...], w_in_ref[step], preferred_element_type=jnp.float32)
        at = pl.multiple_of(step * tile, tile)
        hidden_ref[:, pl.ds(at, tile)] = jnp.maximum(part, 0.0).astype(jnp.bfloat16)

    for copy in lasts:
        copy.wait()
    for at in outs:
        part = lax.dot_general(
            hidden_ref[...],
            w_out_ref[at : at + out_tile],
            (((1,), (1,)), ((), ())),
            preferred_element_type=jnp.float32,
        )
        out_ref[:, :, at : at + out_tile] = part.astype(jnp.bfloat16).reshape(blocks, CAP, out_tile)


def run_expert(rows, near_w_in, w_in, w_out):
    blocks, _, width = rows.shape
    ff = w_in.shape[-1]
    return pl.pallas_call(
        expert_kernel,
        out_shape=(
            pltpu.VMEM(rows.shape, jnp.bfloat16),
            pltpu.VMEM(near_w_in.shape, near_w_in.dtype),
        ),
        in_specs=[VMEM, VMEM, HBM, HBM],
        out_specs=(VMEM, VMEM),
        input_output_aliases={1: 1},
        scratch_shapes=[
            pltpu.VMEM((blocks * CAP, width), jnp.bfloat16),
            pltpu.VMEM((blocks * CAP, ff), jnp.bfloat16),
            pltpu.VMEM((width, ff), w_out.dtype),
            pltpu.SemaphoreType.DMA((LATE_PARTS + 1,)),
        ],
        compiler_params=pltpu.CompilerParams(vmem_limit_bytes=24 * MIB),
        cost_estimate=pl.CostEstimate(
            flops=4 * blocks * CAP * width * ff, bytes_accessed=4 * width * ff, transcendentals=0
        ),
        name="expert_ffn",
    )(rows, near_w_in, in_hbm(w_in), in_hbm(w_out))[0]


def combine_kernel(
    returned_ref, tokens_ref, gates_ref, ids_ref, slots_ref, mixed_hbm, mixed_ref, sems
):
    experts, _, width = returned_ref.shape
    tok_dev = tokens_ref.shape[0]
    owners = position_of(ids_ref[...], RETURN_ORDER, experts)
    index = slot_index(owners, slots_ref).reshape(tok_dev, 1)
    gates = gates_ref[...].reshape(tok_dev, 1)
    returned = returned_ref[...].reshape(experts * CAP, width)
    part = tok_dev // 2
    columns = lax.broadcasted_iota(jnp.int32, (part, experts * CAP), 1)
    copies = []
    for at in range(0, tok_dev, part):
        rows = slice(at, at + part)
        masked = (columns == index[rows]).astype(jnp.float32).astype(jnp.bfloat16)
        picked = jnp.dot(masked, returned, preferred_element_type=jnp.float32)
        mixed = tokens_ref[rows].astype(jnp.float32) + gates[rows] * picked
        mixed_ref[rows] = mixed.astype(jnp.bfloat16)
        copy = pltpu.make_async_copy(mixed_ref.at[rows], mixed_hbm.at[rows], sems.at[at // part])
        copy.start()
        copies.append(copy)
    for copy in copies:
        copy.wait()


def combine(returned, tokens, gates, expert_ids, slots):
    experts, _, width = returned.shape
    tok_dev = tokens.shape[0]
    return pl.pallas_call(
        combine_kernel,
        out_shape=jax.ShapeDtypeStruct(tokens.shape, jnp.bfloat16),
        in_specs=[VMEM] * 5,
        out_specs=HBM,
        scratch_shapes=[
            pltpu.VMEM(tokens.shape, jnp.bfloat16),
            pltpu.SemaphoreType.DMA((2,)),
        ],
        compiler_params=pltpu.CompilerParams(vmem_limit_bytes=8 * MIB),
        cost_estimate=pl.CostEstimate(
            flops=2 * experts * CAP * tok_dev * width,
            bytes_accessed=2 * tok_dev * width,
            transcendentals=0,
        ),
        name="combine",
    )(returned, tokens, gates, expert_ids, slots)


def exchange(blocks, order):
    groups = [members(order, blocks.shape[0])]
    return lax.all_to_all(blocks, AXES, 0, 0, tiled=True, axis_index_groups=groups)


def local(tokens, norm_gain, gates, expert_ids, slots, w_in, w_out):
    experts = lax.axis_size("expert") * lax.axis_size("tensor")
    sent, *kept, near_w_in = dispatch(tokens, norm_gain, gates, expert_ids, slots, w_in, experts)
    result = run_expert(exchange(sent, DISPATCH_ORDER), near_w_in, w_in, w_out)
    return combine(exchange(result, RETURN_ORDER), *kept)


def solution(mesh):
    rows = P(AXES)
    matrix = P(AXES, None)
    weights = P(AXES, None, None)
    return jax.shard_map(
        local,
        mesh=mesh,
        in_specs=(matrix, P(), rows, rows, rows, weights, weights),
        out_specs=matrix,
        check_vma=False,
    )
```
